16 devices in a mesh: dp: 1, tp: 16 (over x, y, z, core).
Axes of the slice: x: 2, y: 2, z: 2, core: 2. Of those that a mesh axis runs over, the one named last changes fastest.
Arguments:
- x: bfloat16 [2048, 4096], P('dp')
- w_gate: bfloat16 [4096, 10240], P(None, 'tp')
- w_up: bfloat16 [4096, 10240], P(None, 'tp')
- w_down: bfloat16 [10240, 4096], P('tp')
Outputs:
- output: bfloat16 [2048, 4096], P('dp')
All inputs are finite; a program needn't handle non-finite values.
Results may differ from the reference program's by a relative error of at most 0.016.
Values are sent between devices in bfloat16 or wider.
A program may use at most 2 GiB of HBM per device.

```python
import jax
import jax.numpy as jnp

ROWS = 2048
D = 4096
FF = 10240


def setup_inputs(seed: int = 0, part: int = 0) -> dict:
    kx, kg, ku, kd = jax.random.split(jax.random.key(seed), 4)
    drawn = {
        "x": jax.random.normal(jax.random.fold_in(kx, part), (ROWS, D), jnp.float32),
        "w_gate": jax.random.normal(kg, (D, FF), jnp.float32) * D**-0.5,
        "w_up": jax.random.normal(ku, (D, FF), jnp.float32) * D**-0.5,
        "w_down": jax.random.normal(kd, (FF, D), jnp.float32) * FF**-0.5,
    }
    return {k: v.astype(jnp.bfloat16) for k, v in drawn.items()}


def reference(x, w_gate, w_up, w_down):
    gate = jnp.dot(x, w_gate, preferred_element_type=jnp.float32)
    up = jnp.dot(x, w_up, preferred_element_type=jnp.float32)
    hidden = (jax.nn.gelu(gate) * up).astype(jnp.bfloat16)
    return jnp.dot(hidden, w_down, preferred_element_type=jnp.float32).astype(jnp.bfloat16)
```

```python
import functools

import jax
import jax.numpy as jnp
from jax import lax
from jax.experimental import pallas as pl
from jax.experimental.pallas import tpu as pltpu
from jax.sharding import PartitionSpec as P

MESH = pl.DeviceIdType.MESH
CHUNKS = 8
RING = 4


def kernel(
    cfg, x_ref, wg_ref, wu_ref, wd_ref, y_ref,
    xb, wgu, wd, h, hs, keep, s1, s2, s3, r1, r2, r3,
    xsem, wsem, wdl, wds, wdr, hss, hsr, ss, rs, fs, fr,
):
    n, R, ff, parts = cfg
    half, quarter, eighth = R // 2, R // 4, R // 8
    me = lax.axis_index("tp")
    core = lax.rem(me, 2)
    bits = (lax.div(me, 8), lax.rem(lax.div(me, 4), 2), lax.rem(lax.div(me, 2), 2))
    strides = (8, 4, 2)
    partner = me + 1 - 2 * core
    across = [me + s * (1 - 2 * b) for s, b in zip(strides, bits)]
    rows = n * R
    mine = core * rows
    other = (1 - core) * rows

    def dev(d):
        return {"tp": d}

    def bit(p, k):
        return bits[(p + k) % 3]

    def to(p, k):
        return dev(across[(p + k) % 3])

    def x_copies(i):
        slot = lax.rem(i, 2)
        return [
            pltpu.make_async_copy(
                x_ref.at[pl.ds(pl.multiple_of(start + i * R, R), R), :],
                xb.at[slot, pl.ds(j * R, R), :],
                xsem.at[slot, j],
            )
            for j, start in enumerate((mine, other))
        ]

    wg_copy = pltpu.make_async_copy(wg_ref, wgu.at[:, pl.ds(0, ff)], wsem.at[0])
    wu_copy = pltpu.make_async_copy(wu_ref, wgu.at[:, pl.ds(ff, ff)], wsem.at[1])
    wd_local = pltpu.make_async_copy(wd_ref, wd.at[pl.ds(0, ff), :], wdl.at[0])

    def wd_swap(p):
        c0, w = parts[p]
        return pltpu.make_async_remote_copy(
            wd_ref.at[:, pl.ds(c0, w)],
            wd.at[pl.ds(ff, ff), pl.ds(c0, w)],
            wds.at[p], wdr.at[p], device_id=dev(partner), device_id_type=MESH,
        )

    def h_swap(i):
        return pltpu.make_async_remote_copy(
            hs.at[lax.rem(i, 2)],
            h.at[i, :, pl.ds(ff, ff)],
            hss.at[i], hsr.at[i], device_id=dev(partner), device_id_type=MESH,
        )

    def y_rows(i, p, depth):
        start = mine + i * R
        size = R
        for k in range(depth):
            size //= 2
            start = start + bit(p, k) * size
        return pl.ds(pl.multiple_of(start, size), size)

    def hop(stage, i, p):
        c0, w = parts[p]
        cols = pl.ds(c0, w)
        slot = lax.rem(i, RING)
        if stage == 0:
            src, dst, k = s1.at[slot, :, cols], r1.at[i, :, cols], 0
        elif stage == 1:
            src, dst, k = s2.at[slot, :, cols], r2.at[i, :, cols], 1
        elif stage == 2:
            src, dst, k = s3.at[slot, :, cols], r3.at[i, :, cols], 2
        else:
            k = 5 - stage
            src = dst = y_ref.at[y_rows(i, p, k + 1), cols]
        return pltpu.make_async_remote_copy(
            src, dst, ss.at[stage, i, p], rs.at[stage, i, p],
            device_id=to(p, k), device_id_type=MESH,
        )

    def forward(i, p, late):
        c0, w = parts[p]
        b = bit(p, 0)
        start = mine + i * R + (1 - b if late else b) * half
        blk = y_ref.at[pl.ds(pl.multiple_of(start, half), half), pl.ds(c0, w)]
        return pltpu.make_async_remote_copy(
            blk, blk, fs.at[late, i, p], fr.at[late, i, p],
            device_id=dev(partner), device_id_type=MESH,
        )

    def gate_up(i):
        slot = lax.rem(i, 2)
        for c in x_copies(i):
            c.wait()
        gu = jnp.dot(xb[slot], wgu[...], preferred_element_type=jnp.float32)
        hid = (jax.nn.gelu(gu[:, :ff]) * gu[:, ff:]).astype(jnp.bfloat16)

        @pl.when(i >= 2)
        def _():
            h_swap(i - 2).wait_send()

        hs[slot] = hid[R:]
        h_swap(i).start()
        h[i, :, pl.ds(0, ff)] = hid[:R]

    def down(i):
        slot = lax.rem(i, RING)
        h_swap(i).wait_recv()
        for p in range(3):
            c0, w = parts[p]

            @pl.when(i == 0)
            def _():
                wd_swap(p).wait_recv()

            term = jnp.dot(
                h[i], wd[:, c0 : c0 + w], preferred_element_type=jnp.float32
            )
            b = bit(p, 0)
            top, bot = term[:half], term[half:]

            @pl.when(i >= RING)
            def _():
                hop(0, i - RING, p).wait_send()

            s1[slot, :, c0 : c0 + w] = jnp.where(b == 1, top, bot).astype(jnp.bfloat16)
            hop(0, i, p).start()
            keep[slot, :, c0 : c0 + w] = jnp.where(b == 1, bot, top)

    def reduce(stage, i):
        slot = lax.rem(i, RING)
        for p in range(3):
            c0, w = parts[p]
            cols = pl.ds(c0, w)
            hop(stage, i, p).wait_recv()
            b1, b2 = bit(p, 1), bit(p, 2)
            if stage == 0:
                o = pl.multiple_of((1 - b1) * quarter, quarter)
                v = keep[slot, pl.ds(o, quarter), cols]
                v = v + r1[i, pl.ds(o, quarter), cols].astype(jnp.float32)

                @pl.when(i >= RING)
                def _():
                    hop(1, i - RING, p).wait_send()

                s2[slot, :, cols] = v.astype(jnp.bfloat16)
                hop(1, i, p).start()
            else:
                b = 1 - b2 if stage == 1 else b2
                o1 = pl.multiple_of(b1 * quarter + b * eighth, eighth)
                o2 = pl.multiple_of(b * eighth, eighth)
                v = keep[slot, pl.ds(o1, eighth), cols]
                v = v + r1[i, pl.ds(o1, eighth), cols].astype(jnp.float32)
                v = v + r2[i, pl.ds(o2, eighth), cols].astype(jnp.float32)
                if stage == 1:

                    @pl.when(i >= RING)
                    def _():
                        hop(2, i - RING, p).wait_send()

                    s3[slot, :, cols] = v.astype(jnp.bfloat16)
                    hop(2, i, p).start()
                else:
                    v = v + r3[i, :, cols].astype(jnp.float32)
                    y_ref[y_rows(i, p, 3), cols] = v.astype(jnp.bfloat16)
                    hop(3, i, p).start()

    def gather(stage, i):
        for p in range(3):
            hop(stage, i, p).wait_recv()
            if stage < 5:
                hop(stage + 1, i, p).start()
            if stage >= 4:
                forward(i, p, stage - 4).start()

    for c in x_copies(0):
        c.start()
    wg_copy.start()
    wu_copy.start()
    wd_local.start()
    barrier = pltpu.get_barrier_semaphore()
    for d in [partner] + across:
        pl.semaphore_signal(barrier, inc=1, device_id=dev(d), device_id_type=MESH)
    pl.semaphore_wait(barrier, 4)
    for p in range(3):
        wd_swap(p).start()
    for c in x_copies(1):
        c.start()
    wg_copy.wait()
    wu_copy.wait()
    gate_up(0)
    wd_local.wait()

    def body(t, _):
        for stage in (5, 4, 3):
            i = t - 1 - stage

            @pl.when(jnp.logical_and(i >= 0, i < n))
            def _():
                gather(stage, i)

        for stage in (2, 1, 0):
            i = t - 1 - stage

            @pl.when(jnp.logical_and(i >= 0, i < n))
            def _():
                reduce(stage, i)

        @pl.when(t < n)
        def _():
            down(t)

        @pl.when(t + 1 < n)
        def _():
            @pl.when(t + 2 < n)
            def _():
                for c in x_copies(t + 2):
                    c.start()

            gate_up(t + 1)

        return 0

    lax.fori_loop(0, n + 6, body, 0)

    for p in range(3):
        wd_swap(p).wait_send()
    for i in range(n - 2, n):
        h_swap(i).wait_send()

    def drain(i, _):
        for p in range(3):
            for stage in range(3, 6):
                hop(stage, i, p).wait_send()
            for late in range(2):
                forward(i, p, late).wait_send()
                forward(i, p, late).wait_recv()
        return 0

    lax.fori_loop(0, n, drain, 0)
    for i in range(n - RING, n):
        for p in range(3):
            for stage in range(3):
                hop(stage, i, p).wait_send()


def solution(mesh):
    def step(x, w_gate, w_up, w_down):
        rows, d = x.shape
        ff = w_gate.shape[1]
        n = CHUNKS
        R = rows // 2 // n
        tiles = d // 128
        widths = [128 * (tiles // 3 + (1 if p < tiles % 3 else 0)) for p in range(3)]
        parts = tuple((sum(widths[:p]), widths[p]) for p in range(3))
        bf16, f32 = jnp.bfloat16, jnp.float32
        dma = pltpu.SemaphoreType.DMA
        return pl.pallas_call(
            functools.partial(kernel, (n, R, ff, parts)),
            name="mlp",
            out_shape=pltpu.VMEM((rows, d), bf16),
            in_specs=[pl.BlockSpec(memory_space=pltpu.HBM)] * 4,
            out_specs=pl.BlockSpec(memory_space=pltpu.VMEM),
            scratch_shapes=[
                pltpu.VMEM((2, 2 * R, d), bf16),
                pltpu.VMEM((d, 2 * ff), bf16),
                pltpu.VMEM((2 * ff, d), bf16),
                pltpu.VMEM((n, R, 2 * ff), bf16),
                pltpu.VMEM((2, R, ff), bf16),
                pltpu.VMEM((RING, R // 2, d), f32),
                pltpu.VMEM((RING, R // 2, d), bf16),
                pltpu.VMEM((RING, R // 4, d), bf16),
                pltpu.VMEM((RING, R // 8, d), bf16),
                pltpu.VMEM((n, R // 2, d), bf16),
                pltpu.VMEM((n, R // 4, d), bf16),
                pltpu.VMEM((n, R // 8, d), bf16),
                dma((2, 2)),
                dma((2,)),
                dma((1,)),
                dma((3,)),
                dma((3,)),
                dma((n,)),
                dma((n,)),
                dma((6, n, 3)),
                dma((6, n, 3)),
                dma((2, n, 3)),
                dma((2, n, 3)),
            ],
            compiler_params=pltpu.CompilerParams(
                collective_id=0,
                has_side_effects=True,
                vmem_limit_bytes=46 * 2**20,
            ),
            cost_estimate=pl.CostEstimate(
                flops=6 * rows * d * ff, bytes_accessed=50 * 2**20, transcendentals=0
            ),
        )(x, w_gate, w_up, w_down)

    return jax.shard_map(
        step,
        mesh=mesh,
        in_specs=(P("dp", None), P(None, "tp"), P(None, "tp"), P("tp", None)),
        out_specs=P("dp", None),
        check_vma=False,
    )
```

```python
import functools

import jax
import jax.numpy as jnp
from jax import lax
from jax.experimental import pallas as pl
from jax.experimental.pallas import tpu as pltpu
from jax.sharding import PartitionSpec as P

MESH = pl.DeviceIdType.MESH
CHUNKS = 8
AHEAD = 2
RINGS = (4, 4, 8)


def kernel(
    cfg, x_ref, wg_ref, wu_ref, wd_ref, y_ref,
    xb, wgu, wd, h, hs, keep, s1, s2, s3, r2, r3,
    xsem, wsem, wdl, wds, wdr, hss, hsr, ss, rs, fs, fr,
):
    n, R, ff, parts = cfg
    half, quarter, eighth = R // 2, R // 4, R // 8
    me = lax.axis_index("tp")
    core = lax.rem(me, 2)
    partner = me + 1 - 2 * core
    rows = n * R
    mine = core * rows
    other = (1 - core) * rows

    def dev(d):
        return {"tp": d}

    def stride(i, p, k):
        a = lax.rem(i + p + k, 3)
        return 8 - 4 * a + a * (a - 1)

    def bit(i, p, k):
        return lax.rem(lax.div(me, stride(i, p, k)), 2)

    def to(i, p, k):
        s = stride(i, p, k)
        return dev(me + s * (1 - 2 * bit(i, p, k)))

    def x_copies(i):
        slot = lax.rem(i, 2)
        return [
            pltpu.make_async_copy(
                x_ref.at[pl.ds(pl.multiple_of(start + i * R, R), R), :],
                xb.at[slot, pl.ds(j * R, R), :],
                xsem.at[slot, j],
            )
            for j, start in enumerate((mine, other))
        ]

    wg_copy = pltpu.make_async_copy(wg_ref, wgu.at[:, pl.ds(0, ff)], wsem.at[0])
    wu_copy = pltpu.make_async_copy(wu_ref, wgu.at[:, pl.ds(ff, ff)], wsem.at[1])
    wd_local = pltpu.make_async_copy(wd_ref, wd.at[pl.ds(0, ff), :], wdl.at[0])

    def wd_swap(p):
        c0, w = parts[p]
        return pltpu.make_async_remote_copy(
            wd_ref.at[:, pl.ds(c0, w)],
            wd.at[pl.ds(ff, ff), pl.ds(c0, w)],
            wds.at[p], wdr.at[p], device_id=dev(partner), device_id_type=MESH,
        )

    def h_swap(i):
        return pltpu.make_async_remote_copy(
            hs.at[lax.rem(i, 2)],
            h.at[i, :, pl.ds(ff, ff)],
            hss.at[i], hsr.at[i], device_id=dev(partner), device_id_type=MESH,
        )

    def y_rows(i, p, depth):
        start = mine + i * R
        size = R
        for k in range(depth):
            size //= 2
            start = start + bit(i, p, k) * size
        return pl.ds(pl.multiple_of(start, size), size)

    def hop(stage, i, p):
        c0, w = parts[p]
        cols = pl.ds(c0, w)
        if stage < 3:
            slot = lax.rem(i, RINGS[stage])
        if stage == 0:
            k = 0
            src = s1.at[slot, :, cols]
            start = mine + i * R + (1 - bit(i, p, 0)) * half
            dst = y_ref.at[pl.ds(pl.multiple_of(start, half), half), cols]
        elif stage == 1:
            src, dst, k = s2.at[slot, :, cols], r2.at[i, :, cols], 1
        elif stage == 2:
            src, dst, k = s3.at[slot, :, cols], r3.at[i, :, cols], 2
        else:
            k = 5 - stage
            src = dst = y_ref.at[y_rows(i, p, k + 1), cols]
        return pltpu.make_async_remote_copy(
            src, dst, ss.at[stage, i, p], rs.at[stage, i, p],
            device_id=to(i, p, k), device_id_type=MESH,
        )

    def forward(i, p, late):
        c0, w = parts[p]
        b = bit(i, p, 0)
        start = mine + i * R + (1 - b if late else b) * half
        blk = y_ref.at[pl.ds(pl.multiple_of(start, half), half), pl.ds(c0, w)]
        return pltpu.make_async_remote_copy(
            blk, blk, fs.at[late, i, p], fr.at[late, i, p],
            device_id=dev(partner), device_id_type=MESH,
        )

    def gate_up(i):
        slot = lax.rem(i, 2)
        for c in x_copies(i):
            c.wait()
        gu = jnp.dot(xb[slot], wgu[...], preferred_element_type=jnp.float32)
        hid = (jax.nn.gelu(gu[:, :ff]) * gu[:, ff:]).astype(jnp.bfloat16)

        @pl.when(i >= 2)
        def _():
            h_swap(i - 2).wait_send()

        hs[slot] = hid[R:]
        h_swap(i).start()
        h[i, :, pl.ds(0, ff)] = hid[:R]

    def down(i):
        slot = lax.rem(i, RINGS[0])
        h_swap(i).wait_recv()
        for p in range(3):
            c0, w = parts[p]

            @pl.when(i == 0)
            def _():
                wd_swap(p).wait_recv()

            term = jnp.dot(
                h[i], wd[:, c0 : c0 + w], preferred_element_type=jnp.float32
            )
            b = bit(i, p, 0)
            top, bot = term[:half], term[half:]

            @pl.when(i >= RINGS[0])
            def _():
                hop(0, i - RINGS[0], p).wait_send()

            s1[slot, :, c0 : c0 + w] = jnp.where(b == 1, top, bot).astype(jnp.bfloat16)
            hop(0, i, p).start()
            keep[i, :, c0 : c0 + w] = jnp.where(b == 1, bot, top)

    def reduce(stage, i):
        for p in range(3):
            c0, w = parts[p]
            cols = pl.ds(c0, w)
            hop(stage, i, p).wait_recv()
            b1, b2 = bit(i, p, 1), bit(i, p, 2)
            kept = mine + i * R + bit(i, p, 0) * half
            if stage == 0:
                o = pl.multiple_of((1 - b1) * quarter, quarter)
                v = keep[i, pl.ds(o, quarter), cols]
                v = v + y_ref[pl.ds(pl.multiple_of(kept + o, quarter), quarter), cols].astype(jnp.float32)

                @pl.when(i >= RINGS[1])
                def _():
                    hop(1, i - RINGS[1], p).wait_send()

                s2[lax.rem(i, RINGS[1]), :, cols] = v.astype(jnp.bfloat16)
                hop(1, i, p).start()
            else:
                b = 1 - b2 if stage == 1 else b2
                o1 = pl.multiple_of(b1 * quarter + b * eighth, eighth)
                o2 = pl.multiple_of(b * eighth, eighth)
                v = keep[i, pl.ds(o1, eighth), cols]
                v = v + y_ref[pl.ds(pl.multiple_of(kept + o1, eighth), eighth), cols].astype(jnp.float32)
                v = v + r2[i, pl.ds(o2, eighth), cols].astype(jnp.float32)
                if stage == 1:

                    @pl.when(i >= RINGS[2])
                    def _():
                        hop(2, i - RINGS[2], p).wait_send()

                    s3[lax.rem(i, RINGS[2]), :, cols] = v.astype(jnp.bfloat16)
                    hop(2, i, p).start()
                else:
                    v = v + r3[i, :, cols].astype(jnp.float32)
                    y_ref[y_rows(i, p, 3), cols] = v.astype(jnp.bfloat16)
                    hop(3, i, p).start()

    def gather(stage, i):
        for p in range(3):
            hop(stage, i, p).wait_recv()
            if stage < 5:
                hop(stage + 1, i, p).start()
            if stage >= 4:
                forward(i, p, stage - 4).start()

    for c in x_copies(0):
        c.start()
    wg_copy.start()
    wu_copy.start()
    wd_local.start()
    barrier = pltpu.get_barrier_semaphore()
    for d in [partner] + [me + s * (1 - 2 * lax.rem(lax.div(me, s), 2)) for s in (8, 4, 2)]:
        pl.semaphore_signal(barrier, inc=1, device_id=dev(d), device_id_type=MESH)
    pl.semaphore_wait(barrier, 4)
    for p in range(3):
        wd_swap(p).start()
    for c in x_copies(1):
        c.start()

    def body(t, _):
        @pl.when(t == 0)
        def _():
            wg_copy.wait()
            wu_copy.wait()

        @pl.when(t == AHEAD)
        def _():
            wd_local.wait()

        @pl.when(jnp.logical_and(t >= AHEAD, t < n + AHEAD))
        def _():
            down(t - AHEAD)

        @pl.when(t < n)
        def _():
            gate_up(t)

            @pl.when(t + 2 < n)
            def _():
                for c in x_copies(t + 2):
                    c.start()

        @pl.when(t > AHEAD)
        def _():
            reduce(0, t - AHEAD - 1)

        return 0

    lax.fori_loop(0, n + AHEAD + 1, body, 0)

    def each(f, stage):
        def body(i, _):
            f(stage, i)
            return 0

        lax.fori_loop(0, n, body, 0)

    for stage in (1, 2):
        each(reduce, stage)
    for stage in (3, 4, 5):
        each(gather, stage)

    for p in range(3):
        wd_swap(p).wait_send()
    for i in range(n - 2, n):
        h_swap(i).wait_send()

    def drain(i, _):
        for p in range(3):
            for stage in range(3, 6):
                hop(stage, i, p).wait_send()
            for late in range(2):
                forward(i, p, late).wait_send()
                forward(i, p, late).wait_recv()
        return 0

    lax.fori_loop(0, n, drain, 0)
    for stage in range(3):
        for i in range(n - RINGS[stage], n):
            for p in range(3):
                hop(stage, i, p).wait_send()


def solution(mesh):
    def step(x, w_gate, w_up, w_down):
        rows, d = x.shape
        ff = w_gate.shape[1]
        n = CHUNKS
        R = rows // 2 // n
        tiles = d // 128
        widths = [128 * (tiles // 3 + (1 if p < tiles % 3 else 0)) for p in range(3)]
        parts = tuple((sum(widths[:p]), widths[p]) for p in range(3))
        bf16, f32 = jnp.bfloat16, jnp.float32
        dma = pltpu.SemaphoreType.DMA
        return pl.pallas_call(
            functools.partial(kernel, (n, R, ff, parts)),
            name="mlp",
            out_shape=pltpu.VMEM((rows, d), bf16),
            in_specs=[pl.BlockSpec(memory_space=pltpu.HBM)] * 4,
            out_specs=pl.BlockSpec(memory_space=pltpu.VMEM),
            scratch_shapes=[
                pltpu.VMEM((2, 2 * R, d), bf16),
                pltpu.VMEM((d, 2 * ff), bf16),
                pltpu.VMEM((2 * ff, d), bf16),
                pltpu.VMEM((n, R, 2 * ff), bf16),
                pltpu.VMEM((2, R, ff), bf16),
                pltpu.VMEM((n, R // 2, d), f32),
                pltpu.VMEM((RINGS[0], R // 2, d), bf16),
                pltpu.VMEM((RINGS[1], R // 4, d), bf16),
                pltpu.VMEM((RINGS[2], R // 8, d), bf16),
                pltpu.VMEM((n, R // 4, d), bf16),
                pltpu.VMEM((n, R // 8, d), bf16),
                dma((2, 2)),
                dma((2,)),
                dma((1,)),
                dma((3,)),
                dma((3,)),
                dma((n,)),
                dma((n,)),
                dma((6, n, 3)),
                dma((6, n, 3)),
                dma((2, n, 3)),
                dma((2, n, 3)),
            ],
            compiler_params=pltpu.CompilerParams(
                collective_id=0,
                has_side_effects=True,
                vmem_limit_bytes=47 * 2**20,
            ),
            cost_estimate=pl.CostEstimate(
                flops=6 * rows * d * ff, bytes_accessed=50 * 2**20, transcendentals=0
            ),
        )(x, w_gate, w_up, w_down)

    return jax.shard_map(
        step,
        mesh=mesh,
        in_specs=(P("dp", None), P(None, "tp"), P(None, "tp"), P("tp", None)),
        out_specs=P("dp", None),
        check_vma=False,
    )
```

```python
import functools

import jax
import jax.numpy as jnp
from jax import lax
from jax.experimental import pallas as pl
from jax.experimental.pallas import tpu as pltpu
from jax.sharding import PartitionSpec as P

MESH = pl.DeviceIdType.MESH
CHUNKS = 8
LAGS = (3, 4, 5, 7, 9)
KEEP = LAGS[2] - 1
RINGS = (4, 4, 8)


def kernel(
    cfg, x_ref, wg_ref, wu_ref, wd_ref, y_ref,
    xb, wgu, wd, h, hs, keep, s1, s2, s3, r2, r3,
    xsem, wsem, wdl, wds, wdr, hss, hsr, ss, rs, fs, fr,
):
    n, R, ff, parts = cfg
    half, quarter, eighth = R // 2, R // 4, R // 8
    me = lax.axis_index("tp")
    core = lax.rem(me, 2)
    partner = me + 1 - 2 * core
    rows = n * R
    mine = core * rows
    other = (1 - core) * rows

    def dev(d):
        return {"tp": d}

    def stride(i, p, k):
        a = lax.rem(i + p + k, 3)
        return 8 - 4 * a + a * (a - 1)

    def bit(i, p, k):
        return lax.rem(lax.div(me, stride(i, p, k)), 2)

    def to(i, p, k):
        s = stride(i, p, k)
        return dev(me + s * (1 - 2 * bit(i, p, k)))

    def x_copies(i):
        slot = lax.rem(i, 2)
        return [
            pltpu.make_async_copy(
                x_ref.at[pl.ds(pl.multiple_of(start + i * R, R), R), :],
                xb.at[slot, pl.ds(j * R, R), :],
                xsem.at[slot, j],
            )
            for j, start in enumerate((mine, other))
        ]

    w_copies = [
        pltpu.make_async_copy(ref, wgu.at[:, pl.ds(j * ff, ff)], wsem.at[j])
        for j, ref in enumerate((wg_ref, wu_ref))
    ]
    wd_local = pltpu.make_async_copy(wd_ref, wd.at[pl.ds(0, ff), :], wdl.at[0])

    def wd_swap(p):
        c0, w = parts[p]
        return pltpu.make_async_remote_copy(
            wd_ref.at[:, pl.ds(c0, w)],
            wd.at[pl.ds(ff, ff), pl.ds(c0, w)],
            wds.at[p], wdr.at[p], device_id=dev(partner), device_id_type=MESH,
        )

    def h_swap(i):
        return pltpu.make_async_remote_copy(
            hs.at[lax.rem(i, 2)],
            h.at[i, :, pl.ds(ff, ff)],
            hss.at[i], hsr.at[i], device_id=dev(partner), device_id_type=MESH,
        )

    def y_rows(i, p, depth):
        start = mine + i * R
        size = R
        for k in range(depth):
            size //= 2
            start = start + bit(i, p, k) * size
        return pl.ds(pl.multiple_of(start, size), size)

    def hop(stage, i, p):
        c0, w = parts[p]
        cols = pl.ds(c0, w)
        if stage < 3:
            slot = lax.rem(i, RINGS[stage])
        if stage == 0:
            k = 0
            src = s1.at[slot, :, cols]
            start = mine + i * R + (1 - bit(i, p, 0)) * half
            dst = y_ref.at[pl.ds(pl.multiple_of(start, half), half), cols]
        elif stage == 1:
            src, dst, k = s2.at[slot, :, cols], r2.at[i, :, cols], 1
        elif stage == 2:
            src, dst, k = s3.at[slot, :, cols], r3.at[i, :, cols], 2
        else:
            k = 5 - stage
            src = dst = y_ref.at[y_rows(i, p, k + 1), cols]
        return pltpu.make_async_remote_copy(
            src, dst, ss.at[stage, i, p], rs.at[stage, i, p],
            device_id=to(i, p, k), device_id_type=MESH,
        )

    def forward(i, p, late):
        c0, w = parts[p]
        b = bit(i, p, 0)
        start = mine + i * R + (1 - b if late else b) * half
        blk = y_ref.at[pl.ds(pl.multiple_of(start, half), half), pl.ds(c0, w)]
        return pltpu.make_async_remote_copy(
            blk, blk, fs.at[late, i, p], fr.at[late, i, p],
            device_id=dev(partner), device_id_type=MESH,
        )

    def dot(a, b):
        return jnp.dot(a, b, preferred_element_type=jnp.float32)

    def hidden(gate, up, i):
        slot = lax.rem(i, 2)
        hid = (jax.nn.gelu(gate) * up).astype(jnp.bfloat16)
        hs[slot] = hid[R:]
        h_swap(i).start()
        h[i, :, pl.ds(0, ff)] = hid[:R]

    def gate_up_first():
        for c in x_copies(0) + w_copies[:1]:
            c.wait()
        gate = dot(xb[0], wgu[:, :ff])
        w_copies[1].wait()
        hidden(gate, dot(xb[0], wgu[:, ff:]), 0)

    def gate_up(i):
        slot = lax.rem(i, 2)
        for c in x_copies(i):
            c.wait()

        @pl.when(i >= 2)
        def _():
            h_swap(i - 2).wait_send()

        gu = dot(xb[slot], wgu[...])
        hidden(gu[:, :ff], gu[:, ff:], i)

    def give(term, i, p):
        c0, w = parts[p]
        b = bit(i, p, 0)
        top, bot = term[:half], term[half:]
        s1[lax.rem(i, RINGS[0]), :, c0 : c0 + w] = jnp.where(b == 1, top, bot).astype(
            jnp.bfloat16
        )
        hop(0, i, p).start()
        keep[lax.rem(i, KEEP), :, c0 : c0 + w] = jnp.where(b == 1, bot, top)

    def down_first():
        h_swap(0).wait_recv()
        wd_local.wait()
        for p in range(3):
            c0, w = parts[p]
            wd_swap(p).wait_recv()
            give(dot(h[0], wd[:, c0 : c0 + w]), 0, p)

    def down(i):
        h_swap(i).wait_recv()

        @pl.when(i >= RINGS[0])
        def _():
            for p in range(3):
                hop(0, i - RINGS[0], p).wait_send()

        term = dot(h[i], wd[...])
        for p in range(3):
            c0, w = parts[p]
            give(term[:, c0 : c0 + w], i, p)

    def reduce(stage, i):
        for p in range(3):
            c0, w = parts[p]
            cols = pl.ds(c0, w)
            hop(stage, i, p).wait_recv()
            b1, b2 = bit(i, p, 1), bit(i, p, 2)
            kept = mine + i * R + bit(i, p, 0) * half
            if stage == 0:
                o = pl.multiple_of((1 - b1) * quarter, quarter)
                v = keep[lax.rem(i, KEEP), pl.ds(o, quarter), cols]
                v = v + y_ref[pl.ds(pl.multiple_of(kept + o, quarter), quarter), cols].astype(jnp.float32)

                @pl.when(i >= RINGS[1])
                def _():
                    hop(1, i - RINGS[1], p).wait_send()

                s2[lax.rem(i, RINGS[1]), :, cols] = v.astype(jnp.bfloat16)
                hop(1, i, p).start()
            else:
                b = 1 - b2 if stage == 1 else b2
                o1 = pl.multiple_of(b1 * quarter + b * eighth, eighth)
                o2 = pl.multiple_of(b * eighth, eighth)
                v = keep[lax.rem(i, KEEP), pl.ds(o1, eighth), cols]
                v = v + y_ref[pl.ds(pl.multiple_of(kept + o1, eighth), eighth), cols].astype(jnp.float32)
                v = v + r2[i, pl.ds(o2, eighth), cols].astype(jnp.float32)
                if stage == 1:

                    @pl.when(i >= RINGS[2])
                    def _():
                        hop(2, i - RINGS[2], p).wait_send()

                    s3[lax.rem(i, RINGS[2]), :, cols] = v.astype(jnp.bfloat16)
                    hop(2, i, p).start()
                else:
                    v = v + r3[i, :, cols].astype(jnp.float32)
                    y_ref[y_rows(i, p, 3), cols] = v.astype(jnp.bfloat16)
                    hop(3, i, p).start()

    def gather(stage, i):
        for p in range(3):
            hop(stage, i, p).wait_recv()
            if stage < 5:
                hop(stage + 1, i, p).start()
            if stage >= 4:
                forward(i, p, stage - 4).start()

    for c in x_copies(0) + w_copies:
        c.start()
    barrier = pltpu.get_barrier_semaphore()
    for d in [partner] + [me + s * (1 - 2 * lax.rem(lax.div(me, s), 2)) for s in (8, 4, 2)]:
        pl.semaphore_signal(barrier, inc=1, device_id=dev(d), device_id_type=MESH)
    pl.semaphore_wait(barrier, 4)
    for p in range(3):
        wd_swap(p).start()
    for c in x_copies(1) + [wd_local]:
        c.start()
    gate_up_first()
    for c in x_copies(2):
        c.start()

    def step(stage, i):
        (reduce if stage < 3 else gather)(stage, i)

    def body(t, _):
        g = jnp.where(t < 2, t, t - 1)

        @pl.when(jnp.logical_and(t != 2, g < n))
        def _():
            gate_up(g)

            @pl.when(g + 2 < n)
            def _():
                for c in x_copies(g + 2):
                    c.start()

        for stage, lag in enumerate(LAGS):

            @pl.when(jnp.logical_and(t >= lag, t - lag < n))
            def _():
                step(stage, t - lag)

        @pl.when(t == 1)
        def _():
            down_first()

        @pl.when(jnp.logical_and(t > 1, t <= n))
        def _():
            down(t - 1)

        return 0

    last = n + LAGS[0] + 4
    lax.fori_loop(1, last, body, 0)

    def each(stage, start):
        def body(i, _):
            step(stage, i)
            return 0

        lax.fori_loop(start, n, body, 0)

    for stage, lag in enumerate(LAGS):
        if last - lag < n:
            each(stage, last - lag)
    each(5, 0)

    for p in range(3):
        wd_swap(p).wait_send()
    for i in range(n - 2, n):
        h_swap(i).wait_send()

    def drain(i, _):
        for p in range(3):
            for stage in range(3, 6):
                hop(stage, i, p).wait_send()
            for late in range(2):
                forward(i, p, late).wait_send()
                forward(i, p, late).wait_recv()
        return 0

    lax.fori_loop(0, n, drain, 0)
    for stage in range(3):
        for i in range(n - RINGS[stage], n):
            for p in range(3):
                hop(stage, i, p).wait_send()


def solution(mesh):
    def step(x, w_gate, w_up, w_down):
        rows, d = x.shape
        ff = w_gate.shape[1]
        n = CHUNKS
        R = rows // 2 // n
        tiles = d // 128
        widths = [128 * (tiles // 3 + (1 if p < tiles % 3 else 0)) for p in range(3)]
        parts = tuple((sum(widths[:p]), widths[p]) for p in range(3))
        bf16, f32 = jnp.bfloat16, jnp.float32
        dma = pltpu.SemaphoreType.DMA
        return pl.pallas_call(
            functools.partial(kernel, (n, R, ff, parts)),
            name="mlp",
            out_shape=pltpu.VMEM((rows, d), bf16),
            in_specs=[pl.BlockSpec(memory_space=pltpu.HBM)] * 4,
            out_specs=pl.BlockSpec(memory_space=pltpu.VMEM),
            scratch_shapes=[
                pltpu.VMEM((2, 2 * R, d), bf16),
                pltpu.VMEM((d, 2 * ff), bf16),
                pltpu.VMEM((2 * ff, d), bf16),
                pltpu.VMEM((n, R, 2 * ff), bf16),
                pltpu.VMEM((2, R, ff), bf16),
                pltpu.VMEM((KEEP, R // 2, d), f32),
                pltpu.VMEM((RINGS[0], R // 2, d), bf16),
                pltpu.VMEM((RINGS[1], R // 4, d), bf16),
                pltpu.VMEM((RINGS[2], R // 8, d), bf16),
                pltpu.VMEM((n, R // 4, d), bf16),
                pltpu.VMEM((n, R // 8, d), bf16),
                dma((2, 2)),
                dma((2,)),
                dma((1,)),
                dma((3,)),
                dma((3,)),
                dma((n,)),
                dma((n,)),
                dma((6, n, 3)),
                dma((6, n, 3)),
                dma((2, n, 3)),
                dma((2, n, 3)),
            ],
            compiler_params=pltpu.CompilerParams(
                collective_id=0,
                has_side_effects=True,
                vmem_limit_bytes=47 * 2**20,
            ),
            cost_estimate=pl.CostEstimate(
                flops=6 * rows * d * ff, bytes_accessed=50 * 2**20, transcendentals=0
            ),
        )(x, w_gate, w_up, w_down)

    return jax.shard_map(
        step,
        mesh=mesh,
        in_specs=(P("dp", None), P(None, "tp"), P(None, "tp"), P("tp", None)),
        out_specs=P("dp", None),
        check_vma=False,
    )
```

```python
import functools

import jax
import jax.numpy as jnp
from jax import lax
from jax.experimental import pallas as pl
from jax.experimental.pallas import tpu as pltpu
from jax.sharding import PartitionSpec as P

MESH = pl.DeviceIdType.MESH
CHUNKS = 8
LAGS = (3, 4, 5, 7, 9)
KEEP = LAGS[2] - 1
RINGS = (4, 4, 8)


def kernel(
    cfg, x_ref, wg_ref, wu_ref, wd_ref, y_ref,
    xb, wgu, wd, h, hs, keep, s1, s2, s3, r2, r3,
    xsem, wsem, wdl, wds, wdr, hss, hsr, ss, rs, gs, fs, fr,
):
    n, R, ff, parts = cfg
    half, quarter, eighth = R // 2, R // 4, R // 8
    me = lax.axis_index("tp")
    core = lax.rem(me, 2)
    partner = me + 1 - 2 * core
    rows = n * R
    mine = core * rows
    other = (1 - core) * rows

    def dev(d):
        return {"tp": d}

    def stride(i, p, k):
        a = lax.rem(i + p + k, 3)
        return 8 - 4 * a + a * (a - 1)

    def bit(i, p, k):
        return lax.rem(lax.div(me, stride(i, p, k)), 2)

    def to(i, p, k):
        s = stride(i, p, k)
        return dev(me + s * (1 - 2 * bit(i, p, k)))

    def x_copies(i):
        slot = lax.rem(i, 2)
        return [
            pltpu.make_async_copy(
                x_ref.at[pl.ds(pl.multiple_of(start + i * R, R), R), :],
                xb.at[slot, pl.ds(j * R, R), :],
                xsem.at[slot, j],
            )
            for j, start in enumerate((mine, other))
        ]

    w_copies = [
        pltpu.make_async_copy(ref, wgu.at[:, pl.ds(j * ff, ff)], wsem.at[j])
        for j, ref in enumerate((wg_ref, wu_ref))
    ]
    wd_local = pltpu.make_async_copy(wd_ref, wd.at[pl.ds(0, ff), :], wdl.at[0])

    def wd_swap(p):
        c0, w = parts[p]
        return pltpu.make_async_remote_copy(
            wd_ref.at[:, pl.ds(c0, w)],
            wd.at[pl.ds(ff, ff), pl.ds(c0, w)],
            wds.at[p], wdr.at[p], device_id=dev(partner), device_id_type=MESH,
        )

    def h_swap(i):
        return pltpu.make_async_remote_copy(
            hs.at[lax.rem(i, 2)],
            h.at[i, :, pl.ds(ff, ff)],
            hss.at[lax.rem(i, 2)], hsr.at[i], device_id=dev(partner), device_id_type=MESH,
        )

    def y_rows(i, p, depth):
        start = mine + i * R
        size = R
        for k in range(depth):
            size //= 2
            start = start + bit(i, p, k) * size
        return pl.ds(pl.multiple_of(start, size), size)

    def hop(stage, i, p):
        c0, w = parts[p]
        cols = pl.ds(c0, w)
        if stage < 3:
            slot = lax.rem(i, RINGS[stage])
            sent = ss.at[sum(RINGS[:stage]) + slot, p]
        if stage == 0:
            k = 0
            src = s1.at[slot, :, cols]
            start = mine + i * R + (1 - bit(i, p, 0)) * half
            dst = y_ref.at[pl.ds(pl.multiple_of(start, half), half), cols]
        elif stage == 1:
            src, dst, k = s2.at[slot, :, cols], r2.at[i, :, cols], 1
        elif stage == 2:
            src, dst, k = s3.at[slot, :, cols], r3.at[i, :, cols], 2
        else:
            k = 5 - stage
            src = dst = y_ref.at[y_rows(i, p, k + 1), cols]
            sent = gs
        return pltpu.make_async_remote_copy(
            src, dst, sent, rs.at[stage, i, p],
            device_id=to(i, p, k), device_id_type=MESH,
        )

    def forward(i, p, late):
        c0, w = parts[p]
        b = bit(i, p, 0)
        start = mine + i * R + (1 - b if late else b) * half
        blk = y_ref.at[pl.ds(pl.multiple_of(start, half), half), pl.ds(c0, w)]
        return pltpu.make_async_remote_copy(
            blk, blk, fs, fr,
            device_id=dev(partner), device_id_type=MESH,
        )

    def dot(a, b):
        return jnp.dot(a, b, preferred_element_type=jnp.float32)

    def hidden(gate, up, i):
        slot = lax.rem(i, 2)
        hid = (jax.nn.gelu(gate) * up).astype(jnp.bfloat16)
        hs[slot] = hid[R:]
        h_swap(i).start()
        h[i, :, pl.ds(0, ff)] = hid[:R]

    def gate_up_first():
        for c in x_copies(0) + w_copies[:1]:
            c.wait()
        for c in [wd_local] + x_copies(1):
            c.start()
        gate = dot(xb[0], wgu[:, :ff])
        w_copies[1].wait()
        hidden(gate, dot(xb[0], wgu[:, ff:]), 0)
        wd_swap(2).start()

    def gate_up(i):
        slot = lax.rem(i, 2)
        for c in x_copies(i):
            c.wait()

        @pl.when(i >= 2)
        def _():
            h_swap(i - 2).wait_send()

        gu = dot(xb[slot], wgu[...])
        hidden(gu[:, :ff], gu[:, ff:], i)

    def give(term, i, p):
        c0, w = parts[p]
        b = bit(i, p, 0)
        top, bot = term[:half], term[half:]
        s1[lax.rem(i, RINGS[0]), :, c0 : c0 + w] = jnp.where(b == 1, top, bot).astype(
            jnp.bfloat16
        )
        hop(0, i, p).start()
        keep[lax.rem(i, KEEP), :, c0 : c0 + w] = jnp.where(b == 1, bot, top)

    def down_first():
        h_swap(0).wait_recv()
        wd_local.wait()
        for p in range(3):
            c0, w = parts[p]
            wd_swap(p).wait_recv()
            give(dot(h[0], wd[:, c0 : c0 + w]), 0, p)

    def down(i):
        h_swap(i).wait_recv()

        @pl.when(i >= RINGS[0])
        def _():
            for p in range(3):
                hop(0, i - RINGS[0], p).wait_send()

        term = dot(h[i], wd[...])
        for p in range(3):
            c0, w = parts[p]
            give(term[:, c0 : c0 + w], i, p)

    def reduce(stage, i):
        for p in range(3):
            c0, w = parts[p]
            cols = pl.ds(c0, w)
            hop(stage, i, p).wait_recv()
            b1, b2 = bit(i, p, 1), bit(i, p, 2)
            kept = mine + i * R + bit(i, p, 0) * half
            if stage == 0:
                o = pl.multiple_of((1 - b1) * quarter, quarter)
                v = keep[lax.rem(i, KEEP), pl.ds(o, quarter), cols]
                v = v + y_ref[pl.ds(pl.multiple_of(kept + o, quarter), quarter), cols].astype(jnp.float32)

                @pl.when(i >= RINGS[1])
                def _():
                    hop(1, i - RINGS[1], p).wait_send()

                s2[lax.rem(i, RINGS[1]), :, cols] = v.astype(jnp.bfloat16)
                hop(1, i, p).start()
            else:
                b = 1 - b2 if stage == 1 else b2
                o1 = pl.multiple_of(b1 * quarter + b * eighth, eighth)
                o2 = pl.multiple_of(b * eighth, eighth)
                v = keep[lax.rem(i, KEEP), pl.ds(o1, eighth), cols]
                v = v + y_ref[pl.ds(pl.multiple_of(kept + o1, eighth), eighth), cols].astype(jnp.float32)
                v = v + r2[i, pl.ds(o2, eighth), cols].astype(jnp.float32)
                if stage == 1:

                    @pl.when(i >= RINGS[2])
                    def _():
                        hop(2, i - RINGS[2], p).wait_send()

                    s3[lax.rem(i, RINGS[2]), :, cols] = v.astype(jnp.bfloat16)
                    hop(2, i, p).start()
                else:
                    v = v + r3[i, :, cols].astype(jnp.float32)
                    y_ref[y_rows(i, p, 3), cols] = v.astype(jnp.bfloat16)
                    hop(3, i, p).start()

    def gather(stage, i):
        for p in range(3):
            hop(stage, i, p).wait_recv()
            if stage < 5:
                hop(stage + 1, i, p).start()
            if stage >= 4:
                forward(i, p, stage - 4).start()

    for c in x_copies(0) + w_copies:
        c.start()
    barrier = pltpu.get_barrier_semaphore()
    for d in [partner] + [me + s * (1 - 2 * lax.rem(lax.div(me, s), 2)) for s in (8, 4, 2)]:
        pl.semaphore_signal(barrier, inc=1, device_id=dev(d), device_id_type=MESH)
    pl.semaphore_wait(barrier, 4)
    for p in range(2):
        wd_swap(p).start()
    gate_up_first()
    for c in x_copies(2):
        c.start()

    def step(stage, i):
        (reduce if stage < 3 else gather)(stage, i)

    def body(t, _):
        g = jnp.where(t < 2, t, t - 1)

        @pl.when(jnp.logical_and(t != 2, g < n))
        def _():
            gate_up(g)

            @pl.when(g + 2 < n)
            def _():
                for c in x_copies(g + 2):
                    c.start()

        for stage, lag in enumerate(LAGS):

            @pl.when(jnp.logical_and(t >= lag, t - lag < n))
            def _():
                step(stage, t - lag)

        @pl.when(t == 1)
        def _():
            down_first()

        @pl.when(jnp.logical_and(t > 1, t <= n))
        def _():
            down(t - 1)

        return 0

    last = n + LAGS[0] + 4
    lax.fori_loop(1, last, body, 0)

    def each(stage, start):
        def body(i, _):
            step(stage, i)
            return 0

        lax.fori_loop(start, n, body, 0)

    for stage, lag in enumerate(LAGS):
        if last - lag < n:
            each(stage, last - lag)
    each(5, 0)

    for p in range(3):
        wd_swap(p).wait_send()
    for i in range(n - 2, n):
        h_swap(i).wait_send()

    def all_of(count, sent, arrived):
        blk = y_ref.at[pl.ds(0, count), :]
        return pltpu.make_async_remote_copy(
            blk, blk, sent, arrived, device_id=dev(partner), device_id_type=MESH
        )

    all_of(rows - rows // 8, gs, fr).wait_send()
    all_of(rows, fs, fr).wait()
    for stage in range(3):
        for i in range(n - RINGS[stage], n):
            for p in range(3):
                hop(stage, i, p).wait_send()


def store(y):
    pieces = 8

    def body(y_ref, o_ref, sem):
        rows = y.shape[0] // pieces
        copies = [
            pltpu.make_async_copy(
                y_ref.at[pl.ds(i * rows, rows)], o_ref.at[pl.ds(i * rows, rows)], sem.at[i]
            )
            for i in range(pieces)
        ]
        for c in copies:
            c.start()
        for c in copies:
            c.wait()

    return pl.pallas_call(
        body,
        name="store",
        out_shape=jax.ShapeDtypeStruct(y.shape, y.dtype),
        in_specs=[pl.BlockSpec(memory_space=pltpu.VMEM)],
        out_specs=pl.BlockSpec(memory_space=pltpu.HBM),
        scratch_shapes=[pltpu.SemaphoreType.DMA((pieces,))],
        compiler_params=pltpu.CompilerParams(vmem_limit_bytes=2**20),
    )(y)


def solution(mesh):
    def step(x, w_gate, w_up, w_down):
        rows, d = x.shape
        ff = w_gate.shape[1]
        n = CHUNKS
        R = rows // 2 // n
        tiles = d // 128
        widths = [128 * (tiles // 3 + (1 if p < tiles % 3 else 0)) for p in range(3)]
        parts = tuple((sum(widths[:p]), widths[p]) for p in range(3))
        bf16, f32 = jnp.bfloat16, jnp.float32
        dma = pltpu.SemaphoreType.DMA
        y = pl.pallas_call(
            functools.partial(kernel, (n, R, ff, parts)),
            name="mlp",
            out_shape=pltpu.VMEM((rows, d), bf16),
            in_specs=[pl.BlockSpec(memory_space=pltpu.HBM)] * 4,
            out_specs=pl.BlockSpec(memory_space=pltpu.VMEM),
            scratch_shapes=[
                pltpu.VMEM((2, 2 * R, d), bf16),
                pltpu.VMEM((d, 2 * ff), bf16),
                pltpu.VMEM((2 * ff, d), bf16),
                pltpu.VMEM((n, R, 2 * ff), bf16),
                pltpu.VMEM((2, R, ff), bf16),
                pltpu.VMEM((KEEP, R // 2, d), f32),
                pltpu.VMEM((RINGS[0], R // 2, d), bf16),
                pltpu.VMEM((RINGS[1], R // 4, d), bf16),
                pltpu.VMEM((RINGS[2], R // 8, d), bf16),
                pltpu.VMEM((n, R // 4, d), bf16),
                pltpu.VMEM((n, R // 8, d), bf16),
                dma((2, 2)),
                dma((2,)),
                dma((1,)),
                dma((3,)),
                dma((3,)),
                dma((2,)),
                dma((n,)),
                dma((sum(RINGS), 3)),
                dma((6, n, 3)),
                dma,
                dma,
                dma,
            ],
            compiler_params=pltpu.CompilerParams(
                collective_id=0,
                has_side_effects=True,
                vmem_limit_bytes=47 * 2**20,
            ),
            cost_estimate=pl.CostEstimate(
                flops=6 * rows * d * ff, bytes_accessed=50 * 2**20, transcendentals=0
            ),
        )(x, w_gate, w_up, w_down)
        return store(y)

    return jax.shard_map(
        step,
        mesh=mesh,
        in_specs=(P("dp", None), P(None, "tp"), P(None, "tp"), P("tp", None)),
        out_specs=P("dp", None),
        check_vma=False,
    )
```
